128 devices in a mesh: row: 16 (over x_hi, y, core), col: 8 (over z, x_lo).
Axes of the slice: x: 4 (x_hi: 2, x_lo: 2; x = x_hi * 2 + x_lo), y: 4, z: 4, core: 2. Of those that a mesh axis runs over, the one named last changes fastest.
Arguments:
- constraint_tiles: float32 [1536, 8, 128, 128], P('row', 'col'), may hold values from -0.25 to 0.25
- constraint_rows: int32 [1536, 8], P('row', 'col'), may hold values from 0 to 191
- constraint_cols: int32 [1536, 8], P('row', 'col'), may hold values from 0 to 255
- factor_tiles: float32 [768, 8, 128, 128], P('row', 'col'), may hold values from -0.21875 to 0.21875
- factor_rows: int32 [768, 8], P('row', 'col'), may hold values from 0 to 63
- factor_cols: int32 [768, 8], P('row', 'col'), may hold values from 0 to 255
- diag_cost: float32 [2048, 128], P('col'), may hold values from 0.1 to 1
- linear_cost: float32 [2048, 128], P('col'), may hold values from -6 to 6
- lower_bound: float32 [3072, 128], P('row'), may hold values from -1.5 to -0.2
- upper_bound: float32 [3072, 128], P('row'), may hold values from 0.2 to 1.5
- primal_start: float32 [2048, 128], P('col'), may hold values from -6 to 6
- slack_start: float32 [3072, 128], P('row'), may hold values from -6 to 6
- dual_start: float32 [3072, 128], P('row'), may hold values from -6 to 6
- penalty: float32 [], replicated, may hold values from 3 to 6
Outputs:
- primal_next: float32 [2048, 128], P('col')
- slack_next: float32 [3072, 128], P('row')
- dual_next: float32 [3072, 128], P('row')
- primal_res: float32 [], replicated
- dual_res: float32 [], replicated
The draws below stay inside these ranges and needn't reach their ends.
All inputs are finite; a program needn't handle non-finite values.
Results may differ from the reference program's by a relative error of at most 0.0003.
Values sent between devices are 32-bit elements; how exact they have to be, the bound alone decides.
A program may use at most 128 MiB of HBM per device.

```python
import math
import jax
import jax.numpy as jnp
from jax import lax

BLK = 128
XB = 256
YB = 192
YG = 64
KA = 96
KG = 48
CG = 6
NX = 2048
NY = 3072
ATILES = 4
GTILES = 6
N_ROW = 16
N_COL = 8


def place_ends(drawn, rng, low, top_value):
    extent = drawn.shape
    index_at = [jax.random.randint(jax.random.fold_in(rng, axis), (), 0, extent[axis]) for axis in range(len(extent))]
    drawn = drawn.at[tuple(index_at)].set(low)
    longest = extent.index(max(extent))
    index_at[longest] = (index_at[longest] + 1) % extent[longest]
    return drawn.at[tuple(index_at)].set(top_value)


def block_scale(rng, shape, cuts, smallest, high):
    level, own = 1.0, jax.random.fold_in(rng, 6)
    for axis_at, parts in cuts:
        steps = jnp.exp(jax.random.uniform(jax.random.fold_in(own, axis_at), (parts,), jnp.float32, smallest / len(cuts), high / len(cuts)))
        level = level * jnp.repeat(steps, shape[axis_at] // parts).reshape([-1 if axis == axis_at else 1 for axis in range(len(shape))])
    return level


def scatter_about(key, extent, scale, reach, split=(), kind=jnp.bfloat16):
    values = scale * jax.random.normal(key, extent, jnp.float32)
    if split:
        values = values * block_scale(key, extent, split, -0.22, 0.18)
    return jnp.clip(values, -reach, reach).astype(kind)


def setup_inputs(seed: int = 0) -> dict:
    key_list = jax.random.split(jax.random.key(seed), 15)
    constraint_tiles = scatter_about(key_list[0], (N_ROW * KA, N_COL, BLK, BLK), (BLK * ATILES) ** -0.5, 0.25, ((0, 16), (1, 8)), jnp.float32)
    constraint_rows = place_ends(jax.random.randint(key_list[1], (N_ROW * KA, N_COL), 0, YB), jax.random.fold_in(key_list[1], 1), 0, YB - 1).astype(jnp.int32)
    constraint_cols = place_ends(jax.random.randint(key_list[2], (N_ROW * KA, N_COL), 0, XB), jax.random.fold_in(key_list[2], 1), 0, XB - 1).astype(jnp.int32)
    factor_tiles = scatter_about(key_list[3], (N_ROW * KG, N_COL, BLK, BLK), (BLK * GTILES) ** -0.5, 0.21875, ((0, 16), (1, 8)), jnp.float32)
    factor_rows = place_ends(jax.random.randint(key_list[4], (N_ROW * KG, N_COL), 0, YG), jax.random.fold_in(key_list[4], 1), 0, YG - 1).astype(jnp.int32)
    factor_cols = place_ends(jax.random.randint(key_list[5], (N_ROW * KG, N_COL), 0, XB), jax.random.fold_in(key_list[5], 1), 0, XB - 1).astype(jnp.int32)
    diag_cost = jnp.clip(jnp.exp(math.log(1.0) - 2.3025851 * jax.random.uniform(key_list[6], (NX, BLK), jnp.float32) ** block_scale(key_list[6], (NX, BLK), ((0, 8),), -0.2, 0.2)), 0.1, 1.0)
    linear_cost = scatter_about(key_list[7], (NX, BLK), 1.0, 6.0, ((0, 8),), jnp.float32)
    lower_bound = jnp.clip(-1.5 + 1.3 * jax.random.uniform(key_list[8], (NY, BLK), jnp.float32) ** block_scale(key_list[8], (NY, BLK), ((0, 16),), -0.2, 0.2), -1.5, -0.2)
    upper_bound = jnp.clip(0.2 + 1.3 * jax.random.uniform(key_list[9], (NY, BLK), jnp.float32) ** block_scale(key_list[9], (NY, BLK), ((0, 16),), -0.2, 0.2), 0.2, 1.5)
    primal_start = scatter_about(key_list[10], (NX, BLK), 1.0, 6.0, ((0, 8),), jnp.float32)
    slack_start = scatter_about(key_list[11], (NY, BLK), 1.0, 6.0, ((0, 16),), jnp.float32)
    dual_start = scatter_about(key_list[12], (NY, BLK), 1.0, 6.0, ((0, 16),), jnp.float32)
    penalty = jnp.clip(jnp.exp(jax.random.uniform(key_list[13], (), jnp.float32, math.log(3.0), math.log(6.0))), 3.0, 6.0)
    return dict(constraint_tiles=constraint_tiles, constraint_rows=constraint_rows, constraint_cols=constraint_cols, factor_tiles=factor_tiles, factor_rows=factor_rows, factor_cols=factor_cols, diag_cost=diag_cost, linear_cost=linear_cost, lower_bound=lower_bound, upper_bound=upper_bound, primal_start=primal_start, slack_start=slack_start, dual_start=dual_start, penalty=penalty)


SIGMA = 1e-6
RELAX = 1.6
HIGH = lax.Precision.HIGHEST


def positions(rows, cols, per_device, row_blocks):
    kidx = jnp.arange(rows.shape[0], dtype=jnp.int32)[:, None] // per_device
    cidx = jnp.arange(rows.shape[1], dtype=jnp.int32)[None, :]
    grow = (kidx * row_blocks + rows).astype(jnp.int32).reshape(-1)
    gcol = (cidx * XB + cols).astype(jnp.int32).reshape(-1)
    return grow, gcol


def forward(tiles, grow, gcol, vec, count):
    prod = jnp.einsum("kij,kj->ki", tiles, vec[gcol], precision=HIGH)
    return jax.ops.segment_sum(prod, grow, num_segments=count)


def backward(tiles, grow, gcol, vec, count):
    prod = jnp.einsum("kij,ki->kj", tiles, vec[grow], precision=HIGH)
    return jax.ops.segment_sum(prod, gcol, num_segments=count)


def reference(constraint_tiles, constraint_rows, constraint_cols, factor_tiles, factor_rows, factor_cols, diag_cost, linear_cost, lower_bound, upper_bound, primal_start, slack_start, dual_start, penalty):
    ctiles = constraint_tiles.reshape(-1, BLK, BLK)
    ftiles = factor_tiles.reshape(-1, BLK, BLK)
    crow, ccol = positions(constraint_rows, constraint_cols, KA, YB)
    frow, fcol = positions(factor_rows, factor_cols, KG, YG)
    nx = XB * N_COL
    ny = YB * N_ROW
    ng = YG * N_ROW
    rho = penalty

    def apply_k(vec):
        avec = forward(ctiles, crow, ccol, vec, ny)
        gvec = forward(ftiles, frow, fcol, vec, ng)
        back = backward(ctiles, crow, ccol, rho * avec, nx) + backward(ftiles, frow, fcol, gvec, nx)
        return (diag_cost + SIGMA) * vec + back

    rhs = SIGMA * primal_start - linear_cost + backward(ctiles, crow, ccol, rho * slack_start - dual_start, nx)
    csq = jax.ops.segment_sum(jnp.sum(ctiles * ctiles, axis=1), ccol, num_segments=nx)
    fsq = jax.ops.segment_sum(jnp.sum(ftiles * ftiles, axis=1), fcol, num_segments=nx)
    precond = diag_cost + SIGMA + fsq + rho * csq
    solution = primal_start
    resid = rhs - apply_k(solution)
    scaled = resid / precond
    direction = scaled
    gamma = jnp.sum(resid * scaled)
    for step in range(CG):
        image = apply_k(direction)
        alpha = gamma / jnp.sum(direction * image)
        solution = solution + alpha * direction
        resid = resid - alpha * image
        scaled = resid / precond
        gamma_new = jnp.sum(resid * scaled)
        direction = scaled + (gamma_new / gamma) * direction
        gamma = gamma_new
    tilde_z = forward(ctiles, crow, ccol, solution, ny)
    primal_next = RELAX * solution + (1.0 - RELAX) * primal_start
    relaxed = RELAX * tilde_z + (1.0 - RELAX) * slack_start
    slack_next = jnp.minimum(jnp.maximum(relaxed + dual_start / rho, lower_bound), upper_bound)
    dual_next = dual_start + rho * (relaxed - slack_next)
    image_next = forward(ctiles, crow, ccol, primal_next, ny)
    gnext = forward(ftiles, frow, fcol, primal_next, ng)
    primal_res = jnp.max(jnp.abs(image_next - slack_next))
    dvec = diag_cost * primal_next + backward(ftiles, frow, fcol, gnext, nx) + linear_cost + backward(ctiles, crow, ccol, dual_next, nx)
    dual_res = jnp.max(jnp.abs(dvec))
    return primal_next, slack_next, dual_next, primal_res, dual_res
```

```python
import functools

import jax
import jax.numpy as jnp
from jax import lax
from jax.experimental import pallas as pl
from jax.experimental.pallas import tpu as pltpu
from jax.sharding import PartitionSpec as P

MESH = pl.DeviceIdType.MESH
YG = 64
CG = 6
SIGMA = 1e-06
RELAX = 1.6
B = 128
TPG = 16
F32 = jnp.float32
BF16 = jnp.bfloat16


def ring_distance(step, size):
    return min(step, size - step)


def peer_offsets(dims, weights):
    offsets = [()]
    for size in dims:
        offsets = [o + (s,) for o in offsets for s in range(size)]
    cost = lambda o: sum(w * ring_distance(s, n) for s, n, w in zip(o, dims, weights))
    return sorted([o for o in offsets if any(o)], key=cost, reverse=True)


def shifted(index, offset, dims, sign):
    out, stride = 0, 1
    for size, step in reversed(list(zip(dims, offset))):
        coord = lax.rem(lax.div(index, jnp.int32(stride)), jnp.int32(size))
        move = step if sign > 0 else (size - step) % size
        coord = lax.rem(coord + jnp.int32(move), jnp.int32(size))
        out = out + coord * jnp.int32(stride)
        stride *= size
    return out


def halves(value):
    high = value.astype(BF16)
    return high, (value - high.astype(F32)).astype(BF16)


def dot(a, b):
    return lax.dot_general(a, b, (((1,), (0,)), ((), ())), preferred_element_type=F32)


class Exchange:
    def __init__(self, axis, index, dims, offsets, sems):
        self.axis, self.index, self.dims, self.offsets, self.sems = axis, index, dims, offsets, sems

    def copy(self, k, src, dst, peer):
        return pltpu.make_async_remote_copy(
            src_ref=src,
            dst_ref=dst,
            send_sem=self.sems.at[0, k],
            recv_sem=self.sems.at[1, k],
            device_id={self.axis: peer},
            device_id_type=MESH,
        )

    def start(self, src_of, dst_of):
        for k, off in enumerate(self.offsets):
            peer = shifted(self.index, off, self.dims, 1)
            self.copy(k, src_of(peer), dst_of(peer), peer).start()

    def wait(self, src_of, dst_from):
        for k, off in enumerate(self.offsets):
            sender = shifted(self.index, off, self.dims, -1)
            self.copy(k, dst_from(sender), dst_from(sender), sender).wait_recv()
        for k, off in enumerate(self.offsets):
            peer = shifted(self.index, off, self.dims, 1)
            self.copy(k, src_of(peer), src_of(peer), peer).wait_send()


def kernel(cfg, ct, ft, idx, diag_in, q_in, x0_in, lb, ub, z0, y0, rho_ref,
           pn_o, sl_o, du_o, res_o,
           raw, tiles, ohc, ohct, ohr, ohrt, lanes_a, lanes_b, part, sqpart,
           ufull, yfull, pfull, xfull, yp, yx, ystart, x0t, prec, dfull, qt, rsh, ssh,
           rcv_c, rcv_r, rcv_q, scal_c, scal_r, scal_m, scal_n,
           load_sems, sem_rc, sem_ac, sem_sc, sem_rr, sem_ar, sem_sr, sem_q, sem_aq, sem_m, sem_n):
    nr, nc, ga, gg, rdims, cdims, roffs, coffs, yb = cfg
    ng = ga + gg
    row = lax.axis_index("row")
    col = lax.axis_index("col")
    jr, ic = B // nr, B // nc
    xw = ufull.shape[1]
    rho = rho_ref[0, 0]

    barrier = pltpu.get_barrier_semaphore()
    for off in roffs:
        pl.semaphore_signal(barrier, inc=1, device_id={"row": shifted(row, off, rdims, 1)}, device_id_type=MESH)
    for off in coffs:
        pl.semaphore_signal(barrier, inc=1, device_id={"col": shifted(col, off, cdims, 1)}, device_id_type=MESH)

    def load(g):
        src = ct.at[pl.ds(g * TPG, TPG)] if g < ga else ft.at[pl.ds((g - ga) * TPG, TPG)]
        return pltpu.make_async_copy(src, raw.at[g], load_sems.at[g])

    for g in range(ng):
        load(g).start()

    def ex(axis, sems):
        if axis == "row":
            return Exchange("row", row, rdims, roffs, sems)
        return Exchange("col", col, cdims, coffs, sems)

    x_rc, x_ac, x_sc = ex("col", sem_rc), ex("col", sem_ac), ex("col", sem_sc)
    x_rr, x_ar, x_sr = ex("row", sem_rr), ex("row", sem_ar), ex("row", sem_sr)
    x_q, x_aq, x_m, x_n = ex("row", sem_q), ex("row", sem_aq), ex("row", sem_m), ex("col", sem_n)

    jrows = lambda i: pl.ds(pl.multiple_of(i * jr, jr), jr)
    irows = lambda i: pl.ds(pl.multiple_of(i * ic, ic), ic)
    mine_j, mine_i = jrows(row), irows(col)

    def transposed(ref, dst):
        for b in range(xw // B):
            dst[:, b * B:(b + 1) * B] = ref[b * B:(b + 1) * B, :].T

    transposed(x0_in, x0t)
    transposed(diag_in, dfull)
    transposed(q_in, qt)

    def onehots(g, _):
        at = pl.ds(pl.multiple_of(g * B, B), B)
        for which, (oh, oht) in enumerate(((ohc, ohct), (ohr, ohrt))):
            ids = jnp.broadcast_to(idx[which, pl.ds(g, 1), :], (B, B))
            wide = jnp.concatenate([ids] * (xw // B), axis=0)
            blocks = lax.broadcasted_iota(jnp.int32, (xw, B), 0).astype(F32)
            oh[:, at] = jnp.where(wide == blocks, 1.0, 0.0).astype(BF16)
            tall = jnp.concatenate([ids.T] * (xw // B), axis=1)
            blocks = lax.broadcasted_iota(jnp.int32, (B, xw), 1).astype(F32)
            oht[at, :] = jnp.where(tall == blocks, 1.0, 0.0).astype(BF16)
        return 0

    lax.fori_loop(0, ng, onehots, 0)

    mask = jnp.where(
        lax.rem(lax.broadcasted_iota(jnp.int32, (8, B), 1), jnp.int32(8)) == lax.broadcasted_iota(jnp.int32, (8, B), 0),
        1.0, 0.0).astype(F32)

    def relayout(g, _):
        pltpu.make_async_copy(ct.at[pl.ds(0, TPG)], raw.at[g], load_sems.at[g]).wait()
        total = jnp.zeros((B, B), F32)
        for i in range(B // 8):
            block = raw[g, :, 8 * i:8 * i + 8, :].reshape(B, B).T
            tiles[g, i] = block
            total = total + block * block
        at = pl.ds(pl.multiple_of(g * B, B), B)
        lanes_b[:, at] = total * jnp.where(g < ga, rho, 1.0)
        return 0

    lax.fori_loop(0, ng, relayout, 0)

    def scatter(lanes, onehot_t, dst):
        high, low = halves(lanes[...])
        dst[...] = dot(high, onehot_t[...]) + dot(low, onehot_t[...])

    def gather(value, onehot, lanes):
        high, low = halves(value)
        lanes[...] = dot(high, onehot[...]) + dot(low, onehot[...])

    def forward(value):
        gather(value, ohc, lanes_a)

        def body(g, _):
            at = pl.ds(pl.multiple_of(g * B, B), B)
            v = lanes_a[:, at]
            for i in range(B // 8):
                prod = (tiles[g, i] * v).reshape(B // 8, 8, B).sum(axis=0)
                lanes_b[8 * i:8 * i + 8, at] = prod.sum(axis=0, keepdims=True) * mask
            return 0

        lax.fori_loop(0, ng, body, 0)
        scatter(lanes_b, ohrt, part)

    def backward(value):
        gather(value, ohr, lanes_a)

        def body(g, _):
            at = pl.ds(pl.multiple_of(g * B, B), B)
            us = [(lanes_a[8 * i:8 * i + 8, at] * mask).sum(axis=0, keepdims=True) for i in range(B // 8)]
            us = [jnp.broadcast_to(u, (8, B)) for u in us]
            for j in range(B // 8):
                acc = tiles[g, 0, 8 * j:8 * j + 8, :] * us[0]
                for i in range(1, B // 8):
                    acc = acc + tiles[g, i, 8 * j:8 * j + 8, :] * us[i]
                lanes_b[8 * j:8 * j + 8, at] = acc
            return 0

        lax.fori_loop(0, ng, body, 0)
        scatter(lanes_b, ohct, part)

    lane_x = lax.broadcasted_iota(jnp.int32, (1, xw), 1)
    weight = jnp.where(lane_x < yb, rho, 1.0)

    def fold(value):
        s = value.sum(axis=0, keepdims=True)
        out = s[:, :B]
        for b in range(1, xw // B):
            out = out + s[:, b * B:(b + 1) * B]
        return out

    def fold_max(value):
        s = value.max(axis=0, keepdims=True)
        out = s[:, :B]
        for b in range(1, xw // B):
            out = jnp.maximum(out, s[:, b * B:(b + 1) * B])
        return out

    def start_rc():
        x_rc.start(lambda p: part.at[irows(p)], lambda p: rcv_c.at[col])

    def finish_rc():
        x_rc.wait(lambda p: part.at[irows(p)], lambda s: rcv_c.at[s])
        total = part[mine_i, :]
        for off in coffs:
            total = total + rcv_c[shifted(col, off, cdims, -1)]
        yfull[mine_i, :] = total
        x_ac.start(lambda p: yfull.at[mine_i], lambda p: yfull.at[mine_i])

    def finish_ac():
        x_ac.wait(lambda p: yfull.at[mine_i], lambda s: yfull.at[irows(s)])

    def start_rr():
        x_rr.start(lambda p: part.at[jrows(p)], lambda p: rcv_r.at[row])

    def finish_rr():
        x_rr.wait(lambda p: part.at[jrows(p)], lambda s: rcv_r.at[s])
        total = part[mine_j, :]
        for off in roffs:
            total = total + rcv_r[shifted(row, off, rdims, -1)]
        return total

    def start_ar(u):
        ufull[mine_j, :] = u
        x_ar.start(lambda p: ufull.at[mine_j], lambda p: ufull.at[mine_j])

    def finish_ar():
        x_ar.wait(lambda p: ufull.at[mine_j], lambda s: ufull.at[jrows(s)])

    scatter(lanes_b, ohct, sqpart)
    pl.semaphore_wait(barrier, len(roffs) + len(coffs))
    x_q.start(lambda p: sqpart.at[jrows(p)], lambda p: rcv_q.at[row])

    forward(x0t[...])
    start_rc()
    x_q.wait(lambda p: sqpart.at[jrows(p)], lambda s: rcv_q.at[s])
    total = sqpart[mine_j, :] + dfull[mine_j, :] + SIGMA
    for off in roffs:
        total = total + rcv_q[shifted(row, off, rdims, -1)]
    prec[mine_j, :] = total
    x_aq.start(lambda p: prec.at[mine_j], lambda p: prec.at[mine_j])

    first = rho * z0[...] - y0[...]
    first = jnp.concatenate([first, jnp.zeros((xw - yb, B), F32)], axis=0)
    for b in range(xw // B):
        yx[:, b * B:(b + 1) * B] = first[b * B:(b + 1) * B, :].T
    finish_rc()
    finish_ac()
    ystart[...] = yfull[...]
    backward(yx[...] - weight * yfull[...])
    start_rr()
    x_aq.wait(lambda p: prec.at[mine_j], lambda s: prec.at[jrows(s)])
    xfull[...] = x0t[...]
    pfull[...] = jnp.zeros_like(pfull)
    yp[...] = jnp.zeros_like(yp)
    yx[...] = ystart[...]
    ssh[...] = jnp.zeros_like(ssh)
    resid = finish_rr() - qt[mine_j, :] - dfull[mine_j, :] * x0t[mine_j, :]
    rsh[...] = resid
    start_ar(resid / prec[mine_j, :])
    finish_ar()

    def first_half(gamma, has_old):
        u = ufull[...]
        square = u * u
        scal_c[col, 0:1, :] = fold(prec[...] * square)
        scal_c[col, 1:2, :] = fold((dfull[...] + SIGMA) * square)
        x_sc.start(lambda p: scal_c.at[col], lambda p: scal_c.at[col])
        forward(u)
        start_rc()
        x_sc.wait(lambda p: scal_c.at[col], lambda s: scal_c.at[s])
        sums = scal_c[...].sum(axis=0)
        sums = sums.sum(axis=1, keepdims=True)
        gamma_new, dx = sums[0:1, :], sums[1:2, :]
        beta = jnp.where(has_old, gamma_new / gamma, 0.0)
        finish_rc()
        pfull[...] = u + beta * pfull[...]
        finish_ac()
        y = yfull[...]
        scal_r[row] = fold(weight * (y * y))
        x_sr.start(lambda p: scal_r.at[row], lambda p: scal_r.at[row])
        return gamma_new, dx, beta

    def step_length(gamma_new, dx, beta, alpha):
        x_sr.wait(lambda p: scal_r.at[row], lambda s: scal_r.at[s])
        delta = dx + scal_r[...].sum(axis=0).sum(axis=1, keepdims=True)
        return gamma_new / (delta - beta * gamma_new / alpha)

    def follow(alpha, beta):
        xfull[...] = xfull[...] + alpha * pfull[...]
        y = yfull[...] + beta * yp[...]
        yp[...] = y
        yx[...] = yx[...] + alpha * y

    def step(t, carry):
        gamma, alpha = carry
        gamma_new, dx, beta = first_half(gamma, t > 0)
        backward(weight * yfull[...])
        start_rr()
        alpha = step_length(gamma_new, dx, beta, alpha)
        u = ufull[mine_j, :]
        image = finish_rr() + (dfull[mine_j, :] + SIGMA) * u
        along = image + beta * ssh[...]
        ssh[...] = along
        resid = rsh[...] - alpha * along
        rsh[...] = resid
        start_ar(resid / prec[mine_j, :])
        follow(alpha, beta)
        finish_ar()
        return gamma_new, alpha

    one = jnp.ones((1, 1), F32)
    gamma, alpha = lax.fori_loop(0, CG - 1, step, (one, one))
    gamma, dx, beta = first_half(gamma, True)
    alpha = step_length(gamma, dx, beta, alpha)
    follow(alpha, beta)

    for b in range(xw // B):
        at = slice(b * B, (b + 1) * B)
        ystart_t = ystart[:, at].T
        yx_t = yx[:, at].T
        rows = min(yb - b * B, B)
        zt = yx_t[:rows]
        rs = slice(b * B, b * B + rows)
        relaxed = RELAX * zt + (1.0 - RELAX) * z0[rs, :]
        dual = y0[rs, :]
        slack = jnp.minimum(jnp.maximum(relaxed + dual / rho, lb[rs, :]), ub[rs, :])
        dual = dual + rho * (relaxed - slack)
        sl_o[rs, :] = slack
        du_o[rs, :] = dual
        image = RELAX * yx_t + (1.0 - RELAX) * ystart_t
        gap = jnp.abs(image[:rows] - slack).max(axis=0, keepdims=True)
        primal = gap if b == 0 else jnp.maximum(primal, gap)
        if rows < B:
            dual = jnp.concatenate([dual, image[rows:]], axis=0)
        yp[:, at] = dual.T
    backward(yp[...])
    start_rr()
    pfull[...] = RELAX * xfull[...] + (1.0 - RELAX) * x0t[...]
    for b in range(xw // B):
        pn_o[b * B:(b + 1) * B, :] = pfull[:, b * B:(b + 1) * B].T
    dvec = finish_rr() + dfull[mine_j, :] * pfull[mine_j, :] + qt[mine_j, :]
    scal_m[row, 0:1, :] = primal
    scal_m[row, 1:2, :] = fold_max(jnp.abs(dvec))
    x_m.start(lambda p: scal_m.at[row], lambda p: scal_m.at[row])
    x_m.wait(lambda p: scal_m.at[row], lambda s: scal_m.at[s])
    scal_n[col] = scal_m[...].max(axis=0)
    x_n.start(lambda p: scal_n.at[col], lambda p: scal_n.at[col])
    x_n.wait(lambda p: scal_n.at[col], lambda s: scal_n.at[s])
    worst = scal_n[...].max(axis=0).max(axis=1, keepdims=True)
    res_o[...] = jnp.broadcast_to(worst, res_o.shape)


def local(dims, ct, crow, ccol, ft, frow, fcol, diag, q, lb, ub, x0, z0, y0, penalty):
    nr, nc, rdims, cdims, rweights, cweights = dims
    ka, kg = ct.shape[0], ft.shape[0]
    ct, ft = ct.reshape(ka, B, B), ft.reshape(kg, B, B)
    ga, gg = ka // TPG, kg // TPG
    ng = ga + gg
    yb = z0.shape[0]
    xw = x0.shape[0]
    cols = jnp.concatenate([ccol.reshape(-1), fcol.reshape(-1)])
    rows = jnp.concatenate([crow.reshape(-1), frow.reshape(-1) + yb])
    idx = jnp.repeat(jnp.stack([cols, rows]).astype(F32), 8, axis=1).reshape(2, ng, B)
    roffs = peer_offsets(rdims, rweights)
    coffs = peer_offsets(cdims, cweights)
    cfg = (nr, nc, ga, gg, rdims, cdims, roffs, coffs, yb)
    lanes = ng * B
    jr, ic = B // nr, B // nc
    vmem = pl.BlockSpec(memory_space=pltpu.VMEM)
    hbm = pl.BlockSpec(memory_space=pl.ANY)
    full = pltpu.VMEM((B, xw), F32)
    dma = pltpu.SemaphoreType.DMA
    csem, rsem = dma((2, len(coffs))), dma((2, len(roffs)))
    outs = pl.pallas_call(
        functools.partial(kernel, cfg),
        out_shape=(
            jax.ShapeDtypeStruct((xw, B), F32),
            jax.ShapeDtypeStruct((yb, B), F32),
            jax.ShapeDtypeStruct((yb, B), F32),
            jax.ShapeDtypeStruct((2, B), F32),
        ),
        in_specs=[hbm, hbm] + [vmem] * 8 + [pl.BlockSpec(memory_space=pltpu.SMEM)],
        out_specs=(vmem,) * 4,
        scratch_shapes=[
            pltpu.VMEM((ng, TPG, B, B), F32),
            pltpu.VMEM((ng, B // 8, B, B), F32),
            pltpu.VMEM((xw, lanes), BF16),
            pltpu.VMEM((lanes, xw), BF16),
            pltpu.VMEM((xw, lanes), BF16),
            pltpu.VMEM((lanes, xw), BF16),
            pltpu.VMEM((B, lanes), F32),
            pltpu.VMEM((B, lanes), F32),
            full, full,
            full, full, full, full, full, full, full, full, full, full, full,
            pltpu.VMEM((jr, xw), F32),
            pltpu.VMEM((jr, xw), F32),
            pltpu.VMEM((nc, ic, xw), F32),
            pltpu.VMEM((nr, jr, xw), F32),
            pltpu.VMEM((nr, jr, xw), F32),
            pltpu.VMEM((nc, 2, B), F32),
            pltpu.VMEM((nr, 1, B), F32),
            pltpu.VMEM((nr, 2, B), F32),
            pltpu.VMEM((nc, 2, B), F32),
            dma((ng,)),
            csem, csem, csem, rsem, rsem, rsem, rsem, rsem, rsem, csem,
        ],
        compiler_params=pltpu.CompilerParams(collective_id=0, has_side_effects=True),
    )(ct, ft, idx, diag, q, x0, lb, ub, z0, y0, penalty.reshape(1, 1))
    pn, sl, du, res = outs
    return pn, sl, du, res[0, 0], res[1, 0]


def solution(mesh):
    nr, nc = mesh.shape["row"], mesh.shape["col"]
    rdims, rweights = ((2, 4, 2), (2, 1, 0)) if nr == 16 else ((nr,), (1,))
    cdims, cweights = ((4, 2), (1, 1)) if nc == 8 else ((nc,), (1,))
    dims = (nr, nc, rdims, cdims, rweights, cweights)
    rc = P("row", "col")
    tiles = P("row", "col", None, None)
    xs, ys = P("col", None), P("row", None)
    return jax.shard_map(
        functools.partial(local, dims),
        mesh=mesh,
        in_specs=(tiles, rc, rc, tiles, rc, rc, xs, xs, ys, ys, xs, ys, ys, P()),
        out_specs=(xs, ys, ys, P(), P()),
        check_vma=False,
    )
```

```python
import functools

import jax
import jax.numpy as jnp
from jax import lax
from jax.experimental import pallas as pl
from jax.experimental.pallas import tpu as pltpu
from jax.sharding import PartitionSpec as P

MESH = pl.DeviceIdType.MESH
YG = 64
CG = 6
SIGMA = 1e-06
RELAX = 1.6
B = 128
TPG = 16
F32 = jnp.float32
BF16 = jnp.bfloat16


def ring_distance(step, size):
    return min(step, size - step)


def peer_offsets(dims, weights):
    offsets = [()]
    for size in dims:
        offsets = [o + (s,) for o in offsets for s in range(size)]
    cost = lambda o: sum(w * ring_distance(s, n) for s, n, w in zip(o, dims, weights))
    return sorted([o for o in offsets if any(o)], key=cost, reverse=True)


def shifted(index, offset, dims, sign):
    out, stride = 0, 1
    for size, step in reversed(list(zip(dims, offset))):
        coord = lax.rem(lax.div(index, jnp.int32(stride)), jnp.int32(size))
        move = step if sign > 0 else (size - step) % size
        coord = lax.rem(coord + jnp.int32(move), jnp.int32(size))
        out = out + coord * jnp.int32(stride)
        stride *= size
    return out


def halves(value):
    high = value.astype(BF16)
    return high, (value - high.astype(F32)).astype(BF16)


def dot(a, b):
    return lax.dot_general(a, b, (((1,), (0,)), ((), ())), preferred_element_type=F32)


class Exchange:
    def __init__(self, axis, targets, senders, sems):
        self.axis, self.targets, self.senders, self.sems = axis, targets, senders, sems

    def copy(self, k, src, dst, peer):
        return pltpu.make_async_remote_copy(
            src_ref=src,
            dst_ref=dst,
            send_sem=self.sems.at[0, k],
            recv_sem=self.sems.at[1, k],
            device_id={self.axis: peer},
            device_id_type=MESH,
        )

    def start(self, src_of, dst_of):
        for k, peer in enumerate(self.targets):
            self.copy(k, src_of(peer), dst_of(peer), peer).start()

    def wait_recv(self, dst_from):
        for k, sender in enumerate(self.senders):
            self.copy(k, dst_from(sender), dst_from(sender), sender).wait_recv()

    def wait_send(self, src_of):
        for k, peer in enumerate(self.targets):
            self.copy(k, src_of(peer), src_of(peer), peer).wait_send()


def kernel(cfg, ct, ft, crow, ccol, frow, fcol, diag_in, q_in, x0_in, lb, ub, z0, y0, rho_ref,
           pn_o, sl_o, du_o, res_o,
           raw, tiles, ohct, ohrt, lane_ids, part, sqpart,
           ufull, yfull, bfull, pfull, xfull, yp, yx, ystart, x0t, prec, dfull, qt, rsh, ssh, gamma_ref, alpha_ref,
           rcv_c, rcv_r, rcv_q, scal_c, scal_r, scal_m, scal_n,
           load_sems, sem_rc, sem_ac, sem_sc, sem_rr, sem_ar, sem_sr, sem_q, sem_aq, sem_m, sem_n):
    nr, nc, ga, gg, rdims, cdims, roffs, coffs, yb = cfg
    ng = ga + gg
    row = lax.axis_index("row")
    col = lax.axis_index("col")
    jr, ic = B // nr, B // nc
    xw = ufull.shape[1]
    rho = rho_ref[0, 0]
    row_targets = [shifted(row, off, rdims, 1) for off in roffs]
    row_senders = [shifted(row, off, rdims, -1) for off in roffs]
    col_targets = [shifted(col, off, cdims, 1) for off in coffs]
    col_senders = [shifted(col, off, cdims, -1) for off in coffs]

    barrier = pltpu.get_barrier_semaphore()
    for peer in row_targets:
        pl.semaphore_signal(barrier, inc=1, device_id={"row": peer}, device_id_type=MESH)
    for peer in col_targets:
        pl.semaphore_signal(barrier, inc=1, device_id={"col": peer}, device_id_type=MESH)

    def load(g):
        src = ct.at[pl.ds(g * TPG, TPG)] if g < ga else ft.at[pl.ds((g - ga) * TPG, TPG)]
        return pltpu.make_async_copy(src, raw.at[g], load_sems.at[g])

    for g in range(ng):
        load(g).start()

    def ex(axis, sems):
        if axis == "row":
            return Exchange("row", row_targets, row_senders, sems)
        return Exchange("col", col_targets, col_senders, sems)

    x_rc, x_ac, x_sc = ex("col", sem_rc), ex("col", sem_ac), ex("col", sem_sc)
    x_rr, x_ar, x_sr = ex("row", sem_rr), ex("row", sem_ar), ex("row", sem_sr)
    x_q, x_aq, x_m, x_n = ex("row", sem_q), ex("row", sem_aq), ex("row", sem_m), ex("col", sem_n)

    jrows = lambda i: pl.ds(pl.multiple_of(i * jr, jr), jr)
    irows = lambda i: pl.ds(pl.multiple_of(i * ic, ic), ic)
    mine_j, mine_i = jrows(row), irows(col)

    def transposed(ref, dst):
        for b in range(xw // B):
            dst[:, b * B:(b + 1) * B] = ref[b * B:(b + 1) * B, :].T

    transposed(x0_in, x0t)
    transposed(diag_in, dfull)
    transposed(q_in, qt)
    ufull[...] = x0t[...]
    xfull[...] = x0t[...]
    pfull[...] = jnp.zeros_like(pfull)
    yp[...] = jnp.zeros_like(yp)
    ssh[...] = jnp.zeros_like(ssh)
    scal_c[...] = jnp.zeros_like(scal_c)
    gamma_ref[...] = jnp.ones_like(gamma_ref)
    alpha_ref[...] = jnp.ones_like(alpha_ref)
    first = rho * z0[...] - y0[...]
    first = jnp.concatenate([first, jnp.zeros((xw - yb, B), F32)], axis=0)
    for b in range(xw // B):
        bfull[:, b * B:(b + 1) * B] = first[b * B:(b + 1) * B, :].T

    def spread(ref, groups):
        count = groups * TPG
        wide = jnp.broadcast_to(ref[...].astype(F32), (16, count))
        own = lax.broadcasted_iota(jnp.int32, (16, count), 1) // TPG == lax.broadcasted_iota(jnp.int32, (16, count), 0)
        pick = lax.rem(lax.broadcasted_iota(jnp.int32, (count, B), 0), jnp.int32(TPG)) == (
            lax.broadcasted_iota(jnp.int32, (count, B), 1) // 8)
        return dot(jnp.where(own, wide, 0.0).astype(BF16), jnp.where(pick, 1.0, 0.0).astype(BF16))

    lane_ids[0, 0:16, :] = spread(ccol, ga)
    lane_ids[0, 16:32, :] = spread(fcol, gg)
    lane_ids[1, 0:16, :] = spread(crow, ga)
    lane_ids[1, 16:32, :] = spread(frow, gg) + float(yb)
    slot = lambda g: g if g < ga else 16 + g - ga

    for which, oht in enumerate((ohct, ohrt)):
        for g in range(ng):
            ids = jnp.broadcast_to(lane_ids[which, slot(g):slot(g) + 1, :], (B, B)).T
            tall = jnp.concatenate([ids] * (xw // B), axis=1)
            blocks = lax.broadcasted_iota(jnp.int32, (B, xw), 1).astype(F32)
            hot = jnp.where(tall == blocks, 1.0, 0.0).astype(BF16)
            oht[g, 0:B, :] = hot
            oht[g, B:2 * B, :] = hot

    mask = jnp.where(
        lax.rem(lax.broadcasted_iota(jnp.int32, (8, B), 1), jnp.int32(8)) == lax.broadcasted_iota(jnp.int32, (8, B), 0),
        1.0, 0.0).astype(F32)

    def scattered(value, onehot_t):
        return dot(jnp.concatenate(halves(value), axis=1), onehot_t)

    def relayout(g, _):
        pltpu.make_async_copy(ct.at[pl.ds(0, TPG)], raw.at[g], load_sems.at[g]).wait()
        total = jnp.zeros((B, B), F32)
        for i in range(B // 8):
            block = raw[g, :, 8 * i:8 * i + 8, :].reshape(B, B).T
            tiles[g, i] = block
            total = total + block * block
        raw[g, 0] = total * jnp.where(g < ga, rho, 1.0)
        return 0

    lax.fori_loop(0, ng, relayout, 0)
    total = scattered(raw[0, 0], ohct[0])
    for g in range(1, ng):
        total = total + scattered(raw[g, 0], ohct[g])
    sqpart[...] = total

    def gathered(ref, which, g):
        ids = jnp.broadcast_to(lane_ids[which, slot(g):slot(g) + 1, :], (8, B)).astype(jnp.int32)
        within = lax.rem(ids, jnp.int32(B))
        out = []
        for i in range(B // 8):
            rows = slice(8 * i, 8 * i + 8)
            value = jnp.take_along_axis(ref[rows, 0:B], within, axis=1)
            for b in range(1, xw // B):
                other = jnp.take_along_axis(ref[rows, b * B:(b + 1) * B], within, axis=1)
                value = jnp.where(ids < b * B, value, other)
            out.append(value)
        return out

    def forward():
        total = None
        for g in range(ng):
            v = gathered(ufull, 0, g)
            rows = []
            for i in range(B // 8):
                prod = tiles[g, i, 0:8, :] * v[0]
                for j in range(1, B // 8):
                    prod = prod + tiles[g, i, 8 * j:8 * j + 8, :] * v[j]
                rows.append(prod.sum(axis=0, keepdims=True) * mask)
            share = scattered(jnp.concatenate(rows, axis=0), ohrt[g])
            total = share if total is None else total + share
        part[...] = total

    def backward():
        total = None
        for g in range(ng):
            us = [(v * mask).sum(axis=0, keepdims=True) for v in gathered(bfull, 1, g)]
            us = [jnp.broadcast_to(u, (8, B)) for u in us]
            rows = []
            for j in range(B // 8):
                acc = tiles[g, 0, 8 * j:8 * j + 8, :] * us[0]
                for i in range(1, B // 8):
                    acc = acc + tiles[g, i, 8 * j:8 * j + 8, :] * us[i]
                rows.append(acc)
            share = scattered(jnp.concatenate(rows, axis=0), ohct[g])
            total = share if total is None else total + share
        part[...] = total

    lane_x = lax.broadcasted_iota(jnp.int32, (1, xw), 1)
    weight = jnp.where(lane_x < yb, rho, 1.0)

    def fold(value):
        s = value.sum(axis=0, keepdims=True)
        out = s[:, :B]
        for b in range(1, xw // B):
            out = out + s[:, b * B:(b + 1) * B]
        return out

    def fold_max(value):
        s = value.max(axis=0, keepdims=True)
        out = s[:, :B]
        for b in range(1, xw // B):
            out = jnp.maximum(out, s[:, b * B:(b + 1) * B])
        return out

    part_i, part_j = (lambda p: part.at[irows(p)]), (lambda p: part.at[jrows(p)])
    sq_j = lambda p: sqpart.at[jrows(p)]
    y_mine, u_mine, prec_mine = (lambda p: yfull.at[mine_i]), (lambda p: ufull.at[mine_j]), (lambda p: prec.at[mine_j])
    sc_mine, sr_mine = (lambda p: scal_c.at[col]), (lambda p: scal_r.at[row])

    def finish_rr():
        x_rr.wait_recv(lambda s: rcv_r.at[s])
        total = part[mine_j, :]
        for sender in row_senders:
            total = total + rcv_r[sender]
        return total

    def step_length(gamma_new, dx, beta):
        x_sr.wait_recv(lambda s: scal_r.at[s])
        delta = dx + scal_r[...].sum(axis=0).sum(axis=1, keepdims=True)
        alpha = gamma_new / (delta - beta * gamma_new / alpha_ref[...])
        alpha_ref[...] = alpha
        x_sr.wait_send(sr_mine)
        return alpha

    def follow(alpha, beta):
        xfull[...] = xfull[...] + alpha * pfull[...]
        y = yfull[...] + beta * yp[...]
        yp[...] = y
        yx[...] = yx[...] + alpha * y

    pl.semaphore_wait(barrier, len(roffs) + len(coffs))
    x_q.start(sq_j, lambda p: rcv_q.at[row])

    last = CG

    def step(t, _):
        @pl.when(t > 0)
        def _():
            u = ufull[...]
            square = u * u
            scal_c[col, 0:1, :] = fold(prec[...] * square)
            scal_c[col, 1:2, :] = fold((dfull[...] + SIGMA) * square)
            x_sc.start(sc_mine, sc_mine)

        forward()
        x_rc.start(part_i, lambda p: rcv_c.at[col])

        @pl.when(t == 0)
        def _():
            x_q.wait_recv(lambda s: rcv_q.at[s])
            total = sqpart[mine_j, :] + dfull[mine_j, :] + SIGMA
            for sender in row_senders:
                total = total + rcv_q[sender]
            prec[mine_j, :] = total
            x_aq.start(prec_mine, prec_mine)
            x_q.wait_send(sq_j)

        @pl.when(t > 0)
        def _():
            x_sc.wait_recv(lambda s: scal_c.at[s])
            x_sc.wait_send(sc_mine)

        sums = scal_c[...].sum(axis=0)
        sums = sums.sum(axis=1, keepdims=True)
        gamma_new, dx = sums[0:1, :], sums[1:2, :]
        beta = jnp.where(t > 1, gamma_new / gamma_ref[...], 0.0)
        gamma_ref[...] = gamma_new

        x_rc.wait_recv(lambda s: rcv_c.at[s])
        total = part[mine_i, :]
        for sender in col_senders:
            total = total + rcv_c[sender]
        yfull[mine_i, :] = total
        x_ac.start(y_mine, y_mine)
        x_rc.wait_send(part_i)
        pfull[...] = ufull[...] + beta * pfull[...]
        x_ac.wait_recv(lambda s: yfull.at[irows(s)])

        @pl.when(t == 0)
        def _():
            y = yfull[...]
            ystart[...] = y
            yx[...] = y
            bfull[...] = bfull[...] - weight * y

        @pl.when(t > 0)
        def _():
            y = yfull[...]
            wy = weight * y
            bfull[...] = wy
            scal_r[row] = fold(wy * y)
            x_sr.start(sr_mine, sr_mine)

        @pl.when(t == last)
        def _():
            follow(step_length(gamma_new, dx, beta), beta)
            for b in range(xw // B):
                at = slice(b * B, (b + 1) * B)
                rows = min(yb - b * B, B)
                rs = slice(b * B, b * B + rows)
                yx_t = yx[:, at].T
                relaxed = RELAX * yx_t[:rows] + (1.0 - RELAX) * z0[rs, :]
                dual = y0[rs, :]
                slack = jnp.minimum(jnp.maximum(relaxed + dual / rho, lb[rs, :]), ub[rs, :])
                dual = dual + rho * (relaxed - slack)
                sl_o[rs, :] = slack
                du_o[rs, :] = dual
                image = RELAX * yx_t + (1.0 - RELAX) * ystart[:, at].T
                gap = jnp.abs(image[:rows] - slack).max(axis=0, keepdims=True)
                primal = gap if b == 0 else jnp.maximum(primal, gap)
                if rows < B:
                    dual = jnp.concatenate([dual, image[rows:]], axis=0)
                bfull[:, at] = dual.T
            scal_m[row, 0:1, :] = primal

        x_ac.wait_send(y_mine)
        backward()
        x_rr.start(part_j, lambda p: rcv_r.at[row])

        @pl.when(t == 0)
        def _():
            x_aq.wait_recv(lambda s: prec.at[jrows(s)])
            x_aq.wait_send(prec_mine)
            resid = finish_rr() - qt[mine_j, :] - dfull[mine_j, :] * x0t[mine_j, :]
            rsh[...] = resid
            ufull[mine_j, :] = resid / prec[mine_j, :]

        @pl.when(jnp.logical_and(t > 0, t < last))
        def _():
            alpha = step_length(gamma_new, dx, beta)
            image = (dfull[mine_j, :] + SIGMA) * ufull[mine_j, :] + beta * ssh[...]
            along = finish_rr() + image
            ssh[...] = along
            resid = rsh[...] - alpha * along
            rsh[...] = resid
            ufull[mine_j, :] = resid / prec[mine_j, :]

        @pl.when(t < last)
        def _():
            x_ar.start(u_mine, u_mine)
            x_rr.wait_send(part_j)

            @pl.when(t > 0)
            def _():
                follow(alpha_ref[...], beta)

            x_ar.wait_recv(lambda s: ufull.at[jrows(s)])
            x_ar.wait_send(u_mine)

        return 0

    lax.fori_loop(0, last + 1, step, 0)
    pfull[...] = RELAX * xfull[...] + (1.0 - RELAX) * x0t[...]
    for b in range(xw // B):
        pn_o[b * B:(b + 1) * B, :] = pfull[:, b * B:(b + 1) * B].T
    known = dfull[mine_j, :] * pfull[mine_j, :] + qt[mine_j, :]
    dvec = finish_rr() + known
    scal_m[row, 1:2, :] = fold_max(jnp.abs(dvec))
    sm_mine, sn_mine = (lambda p: scal_m.at[row]), (lambda p: scal_n.at[col])
    x_m.start(sm_mine, sm_mine)
    x_rr.wait_send(part_j)
    x_m.wait_recv(lambda s: scal_m.at[s])
    scal_n[col] = scal_m[...].max(axis=0)
    x_n.start(sn_mine, sn_mine)
    x_m.wait_send(sm_mine)
    x_n.wait_recv(lambda s: scal_n.at[s])
    x_n.wait_send(sn_mine)
    worst = scal_n[...].max(axis=0).max(axis=1, keepdims=True)
    res_o[...] = jnp.broadcast_to(worst, res_o.shape)


def hand_over(pn, sl, du, res, pn_o, sl_o, du_o, primal_o, dual_o):
    pn_o[...] = pn[...]
    sl_o[...] = sl[...]
    du_o[...] = du[...]
    primal_o[...] = res[0:1, 0:1]
    dual_o[...] = res[1:2, 0:1]


def local(dims, ct, crow, ccol, ft, frow, fcol, diag, q, lb, ub, x0, z0, y0, penalty):
    nr, nc, rdims, cdims, rweights, cweights = dims
    ka, kg = ct.shape[0], ft.shape[0]
    ct, ft = ct.reshape(ka, B, B), ft.reshape(kg, B, B)
    ga, gg = ka // TPG, kg // TPG
    ng = ga + gg
    yb = z0.shape[0]
    xw = x0.shape[0]
    roffs = peer_offsets(rdims, rweights)
    coffs = peer_offsets(cdims, cweights)
    cfg = (nr, nc, ga, gg, rdims, cdims, roffs, coffs, yb)
    jr, ic = B // nr, B // nc
    vmem = pl.BlockSpec(memory_space=pltpu.VMEM)
    hbm = pl.BlockSpec(memory_space=pl.ANY)
    full = pltpu.VMEM((B, xw), F32)
    dma = pltpu.SemaphoreType.DMA
    csem, rsem = dma((2, len(coffs))), dma((2, len(roffs)))
    shapes = [jax.ShapeDtypeStruct(s, F32) for s in ((xw, B), (yb, B), (yb, B), (2, B))]
    outs = pl.pallas_call(
        functools.partial(kernel, cfg),
        out_shape=shapes,
        in_specs=[hbm, hbm] + [vmem] * 11 + [pl.BlockSpec(memory_space=pltpu.SMEM)],
        out_specs=[vmem] * 4,
        scratch_shapes=[
            pltpu.VMEM((ng, TPG, B, B), F32),
            pltpu.VMEM((ng, B // 8, B, B), F32),
            pltpu.VMEM((ng, 2 * B, xw), BF16),
            pltpu.VMEM((ng, 2 * B, xw), BF16),
            pltpu.VMEM((2, 32, B), F32),
            full, full,
            full, full, full, full, full, full, full, full, full, full, full, full,
            pltpu.VMEM((jr, xw), F32),
            pltpu.VMEM((jr, xw), F32),
            pltpu.VMEM((1, 1), F32),
            pltpu.VMEM((1, 1), F32),
            pltpu.VMEM((nc, ic, xw), F32),
            pltpu.VMEM((nr, jr, xw), F32),
            pltpu.VMEM((nr, jr, xw), F32),
            pltpu.VMEM((nc, 2, B), F32),
            pltpu.VMEM((nr, 1, B), F32),
            pltpu.VMEM((nr, 2, B), F32),
            pltpu.VMEM((nc, 2, B), F32),
            dma((ng,)),
            csem, csem, csem, rsem, rsem, rsem, rsem, rsem, rsem, csem,
        ],
        compiler_params=pltpu.CompilerParams(collective_id=0, has_side_effects=True),
    )(ct, ft, crow.reshape(1, ka), ccol.reshape(1, ka), frow.reshape(1, kg), fcol.reshape(1, kg),
      diag, q, x0, lb, ub, z0, y0, penalty.reshape(1, 1))
    one = jax.ShapeDtypeStruct((1, 1), F32)
    pn, sl, du, primal, dual = pl.pallas_call(
        hand_over,
        out_shape=shapes[:3] + [one, one],
        in_specs=[vmem] * 4,
        out_specs=[vmem] * 5,
    )(*outs)
    return pn, sl, du, primal[0, 0], dual[0, 0]


def solution(mesh):
    nr, nc = mesh.shape["row"], mesh.shape["col"]
    rdims, rweights = ((2, 4, 2), (2, 1, 0)) if nr == 16 else ((nr,), (1,))
    cdims, cweights = ((4, 2), (1, 1)) if nc == 8 else ((nc,), (1,))
    dims = (nr, nc, rdims, cdims, rweights, cweights)
    rc = P("row", "col")
    tiles = P("row", "col", None, None)
    xs, ys = P("col", None), P("row", None)
    return jax.shard_map(
        functools.partial(local, dims),
        mesh=mesh,
        in_specs=(tiles, rc, rc, tiles, rc, rc, xs, xs, ys, ys, xs, ys, ys, P()),
        out_specs=(xs, ys, ys, P(), P()),
        check_vma=False,
    )
```
